128 devices in a mesh: dp: 1, tp: 2 (over core), fsdp: 64 (over z, y, x).
Axes of the slice: x: 4, y: 4, z: 4, core: 2. Of those that a mesh axis runs over, the one named last changes fastest.
Arguments:
- tokens: int32 [128, 2048], P(('dp', 'fsdp'))
- out_grad: bfloat16 [128, 2048, 1024], P(('dp', 'fsdp'))
- head_grad: float32 [32128, 1024], P(('dp', 'tp'), 'fsdp')
- master_w: float32 [32128, 1024], P(('dp', 'tp'), 'fsdp')
- moment_m: float32 [32128, 1024], P(('dp', 'tp'), 'fsdp')
- moment_v: float32 [32128, 1024], P(('dp', 'tp'), 'fsdp')
- learn_rate: float32 [], replicated
- clip_scale: float32 [], replicated
Outputs:
- output 1: float32 [32128, 1024], P(('dp', 'tp'), 'fsdp')
- output 2: float32 [32128, 1024], P(('dp', 'tp'), 'fsdp')
- output 3: float32 [32128, 1024], P(('dp', 'tp'), 'fsdp')
- output 4: bfloat16 [32128, 1024], P(('dp', 'tp'), 'fsdp')
All inputs are finite; a program needn't handle non-finite values.
Results may differ from the reference program's by a relative error of at most 0.001.
Values sent between devices are 32-bit elements.
A program may use at most 1 GiB of HBM per device.

```python
import math
import jax
import jax.numpy as jnp

VOCAB_SIZE = 32128
MODEL_DIM = 1024
BATCH_ROWS = 128
SEQ_LEN = 2048
OPT_STEP = 20
TOKEN_LEVELS = int(math.ceil(math.log2(VOCAB_SIZE)))


def draw_tokens(tok_key):
    level_key, value_key, shift_key = jax.random.split(tok_key, 3)
    tok_shape = (BATCH_ROWS, SEQ_LEN)
    levels = jax.random.randint(level_key, tok_shape, 0, TOKEN_LEVELS + 1, dtype=jnp.int32)
    widths = jnp.minimum(jnp.left_shift(jnp.int32(1), levels), VOCAB_SIZE)
    raw_ids = jax.random.randint(value_key, tok_shape, 0, 2 ** 30, dtype=jnp.int32) % widths
    token_shift = jax.random.randint(shift_key, (), 0, VOCAB_SIZE, dtype=jnp.int32)
    tokens = (raw_ids + token_shift) % VOCAB_SIZE
    return tokens.at[0, 0].set(0).at[0, 1].set(VOCAB_SIZE - 1)


def setup_inputs(seed: int = 0, part: int = 0) -> dict:
    base_key = jax.random.key(seed)
    part_key = jax.random.fold_in(base_key, part)
    tok_key, grad_key, head_key, emb_key, mom_key, vel_key = jax.random.split(part_key, 6)
    lr_key, clip_key = jax.random.split(base_key, 2)
    table_shape = (VOCAB_SIZE, MODEL_DIM)
    tokens = draw_tokens(tok_key)
    out_grad = jax.random.normal(grad_key, (BATCH_ROWS, SEQ_LEN, MODEL_DIM), jnp.float32).astype(jnp.bfloat16)
    head_grad = 0.25 * jax.random.normal(head_key, table_shape, jnp.float32)
    master_w = MODEL_DIM ** -0.5 * jax.random.normal(emb_key, table_shape, jnp.float32)
    moment_m = 0.3 * jax.random.normal(mom_key, table_shape, jnp.float32)
    moment_v = 0.0625 * (0.5 + jax.random.uniform(vel_key, table_shape, jnp.float32))
    learn_rate = 0.01 + 0.04 * jax.random.uniform(lr_key, (), jnp.float32)
    clip_scale = 0.5 + 0.5 * jax.random.uniform(clip_key, (), jnp.float32)
    return {"tokens": tokens, "out_grad": out_grad, "head_grad": head_grad, "master_w": master_w, "moment_m": moment_m, "moment_v": moment_v, "learn_rate": learn_rate, "clip_scale": clip_scale}


def reference(tokens, out_grad, head_grad, master_w, moment_m, moment_v, learn_rate, clip_scale):
    beta_two = 1.0 - OPT_STEP ** -0.8
    flat_rows = out_grad.reshape(-1, MODEL_DIM).astype(jnp.float32)
    embed_grad = jax.ops.segment_sum(flat_rows, tokens.reshape(-1), num_segments=VOCAB_SIZE)
    grad_full = clip_scale * (embed_grad + head_grad)
    new_v = beta_two * moment_v + (1.0 - beta_two) * (grad_full * grad_full + 1e-30)
    update = grad_full / jnp.sqrt(new_v)
    new_m = 0.9 * moment_m + 0.1 * update
    new_w = master_w - learn_rate * new_m - learn_rate * learn_rate * master_w
    return (new_w, new_m, new_v, new_w.astype(jnp.bfloat16))
```

```python
import functools

import jax
import jax.numpy as jnp
from jax import lax
from jax.experimental import pallas as pl
from jax.experimental.pallas import tpu as pltpu
from jax.sharding import PartitionSpec as P

OPT_STEP = 20
F32, BF16, I32 = jnp.float32, jnp.bfloat16, jnp.int32
CAP = (480, 352, 208)
KW = 512
STRIDES = ((1, 16), (4, 1), (16, 4))
VLIM = 48 << 20


def update_math(embed_grad, head_grad, master_w, moment_m, moment_v, learn_rate, clip_scale):
    beta_two = 1.0 - OPT_STEP ** -0.8
    grad_full = clip_scale * (embed_grad + head_grad)
    new_v = beta_two * moment_v + (1.0 - beta_two) * (grad_full * grad_full + 1e-30)
    new_m = 0.9 * moment_m + 0.1 * (grad_full / jnp.sqrt(new_v))
    new_w = master_w - learn_rate * new_m - learn_rate * learn_rate * master_w
    return new_w, new_m, new_v


def iota(shape, dim):
    return lax.broadcasted_iota(I32, shape, dim)


def onehot(cond):
    return jnp.where(cond, 1.0, 0.0).astype(BF16)


def dot_nt(a, b):
    return lax.dot_general(a, b, (((1,), (1,)), ((), ())), preferred_element_type=F32)


def dot_nn(a, b):
    return jnp.dot(a, b, preferred_element_type=F32)


def ranks(pres, group):
    rows = pres.shape[0]
    pres_b = pres.astype(BF16)
    before = onehot(iota((KW, KW), 0) < iota((KW, KW), 1))
    inner = dot_nn(pres_b, before)
    if group > 1:
        r, c = iota((rows, rows), 0), iota((rows, rows), 1)
        above = onehot((c < r) & (c // group == r // group))
        inner = inner + jnp.sum(dot_nn(above, pres_b), axis=1, keepdims=True)
    return inner.astype(I32)


def codes(pres, group, cap):
    rows = pres.shape[0]
    rank = ranks(pres, group)
    code = jnp.where((pres > 0.5) & (rank < cap), (iota((rows, KW), 0) // group) * cap + rank + 1, 0)
    over = jnp.where((pres > 0.5) & (rank >= cap), 1.0, 0.0)
    return code, jnp.max(over)


def index_first(coord_ref, tok_ref, slot_ref, pres_ref, over_ref):
    ids = tok_ref[...]
    tp, c1, c2, c3 = (coord_ref[n] for n in range(4))
    x, y, z = ids & 3, (ids >> 2) & 3, (ids >> 4) & 3
    first = jnp.broadcast_to(tp == 0, ids.shape)
    d1 = jnp.where(first, x, z)
    d2 = jnp.where(first, y, x)
    d3 = jnp.where(first, z, y)
    q = (((d1 - c1) & 3) << 4) + (((d2 - c2) & 3) << 2) + ((d3 - c3) & 3)
    upper = ids >= 16064
    kk = jnp.where(upper, ids - 16064, ids) >> 6
    k = jnp.where(upper, 256, 0) + ((kk & 1) << 7) + (kk >> 1)
    n = ids.shape[1]
    hot_q = onehot(iota((64, n), 0) == q)
    hot_k = onehot(iota((KW, n), 0) == k)
    pres = jnp.minimum(dot_nt(hot_q, hot_k), 1.0)
    code, over = codes(pres, 16, CAP[0])
    both = jnp.concatenate([(code >> 5).astype(BF16), (code & 31).astype(BF16)], axis=0)
    found = dot_nn(both, hot_k)
    value = found[:64] * 32.0 + found[64:]
    slot_ref[...] = jnp.sum(jnp.where(iota((64, n), 0) == q, value, 0.0), axis=0, keepdims=True).astype(I32) - 1
    pres_ref[...] = pres
    over_ref[...] = jnp.full(over_ref.shape, over, F32)


def gather_first(o, tp_ref, slot_ref, rows_ref, out_ref):
    cap, depth = out_ref.shape[0], rows_ref.shape[0]
    hot = onehot(iota((cap, depth), 0) == slot_ref[...] - o * cap)
    part = dot_nn(hot, rows_ref[...])

    @pl.when(pl.program_id(0) == 0)
    def _():
        out_ref[...] = part

    @pl.when(pl.program_id(0) > 0)
    def _():
        out_ref[...] += part


def index_next(group, cap_in, cap_out, p0, p1, p2, p3, over_in, slot_ref, pres_ref, over_ref):
    blocks = [p[...] for p in (p0, p1, p2, p3)]
    merged = jnp.minimum(blocks[0] + blocks[1] + blocks[2] + blocks[3], 1.0)
    rows = merged.shape[0]
    code, over = codes(merged, group, cap_out)
    hi, lo = (code >> 5).astype(F32), (code & 31).astype(F32)
    lanes = iota((32, KW), 1)
    spread = onehot((lanes & 31) == iota((32, KW), 0))
    own_row = (iota((16, KW), 1) >> 5) == iota((16, KW), 0)
    for s, pres in enumerate(blocks):
        rank = jnp.where(pres > 0.5, ranks(pres, rows), -1)
        table = jnp.zeros((16, 64), F32)
        for r in range(rows):
            row = rank[r:r + 1]
            high = onehot(iota((16, KW), 0) == (row >> 5))
            low = iota((32, KW), 0) == (row & 31)
            low = jnp.concatenate([jnp.where(low, hi[r:r + 1], 0.0), jnp.where(low, lo[r:r + 1], 0.0)], axis=0)
            table = table + dot_nt(high, low.astype(BF16))
        table = table.astype(BF16)
        value = dot_nn(table[:, :32], spread) * 32.0 + dot_nn(table[:, 32:], spread)
        slot_ref[s:s + 1, :] = jnp.sum(jnp.where(own_row, value, 0.0), axis=0, keepdims=True).astype(I32) - 1
    pres_ref[...] = merged
    over_ref[...] = jnp.maximum(over_in[...], over)


def split_rows(rows):
    high = jnp.clip(rows, -3.38e38, 3.38e38).astype(BF16)
    rest = rows - high.astype(F32)
    mid = rest.astype(BF16)
    return high, mid, (rest - mid.astype(F32)).astype(BF16)


def gather_next(o, slot_ref, r0, r1, r2, r3, out_ref):
    cap_out, cap_in = out_ref.shape[0], r0.shape[0]
    total = None
    for s, rows in enumerate((r0, r1, r2, r3)):
        hot = onehot(iota((cap_out, cap_in), 0) == slot_ref[s:s + 1, :cap_in] - o * cap_out)
        for piece in split_rows(rows[...]):
            part = dot_nn(hot, piece)
            total = part if total is None else total + part
    out_ref[...] = total


def dense_last(p0, p1, p2, p3, r0, r1, r2, r3, over_ref, out_ref):
    total = None
    for pres_ref, rows in ((p0, r0), (p1, r1), (p2, r2), (p3, r3)):
        pres = pres_ref[...]
        rank = jnp.where(pres > 0.5, ranks(pres, 1), -1)[0:1]
        hot = onehot(iota((rows.shape[0], KW), 0) == rank)
        for piece in split_rows(rows[...].T):
            part = dot_nn(piece, hot)
            total = part if total is None else total + part
    flag = over_ref[0:1, 0:1]
    out_ref[...] = jnp.where((iota(total.shape, 1) & 255) == 127 + 128, flag, total)


def finish(scal_ref, recv_ref, head_ref, w_ref, m_ref, v_ref, w_out, m_out, v_out, b_out, grad):
    tiles = grad.shape[0]
    for c in range(16):
        both = jnp.concatenate([recv_ref[:, c, :128], recv_ref[:, c, 128:]], axis=0)
        grad[:, c, :] = both.T[:tiles]
    lr, clip = scal_ref[0], scal_ref[1]
    rows = head_ref.shape[1]
    for t in range(tiles):
        at = slice(128 * t, min(128 * t + 128, rows))
        width = at.stop - at.start
        new_w, new_m, new_v = update_math(grad[t, :, :width], head_ref[:, at], w_ref[:, at], m_ref[:, at], v_ref[:, at], lr, clip)
        w_out[:, at], m_out[:, at], v_out[:, at] = new_w, new_m, new_v
        b_out[:, at] = new_w.astype(BF16)


def call(kernel, name, outs, args, flops, smem=()):
    specs = [pl.BlockSpec(memory_space=pltpu.SMEM if n in smem else pltpu.VMEM) for n in range(len(args))]
    return pl.pallas_call(
        kernel,
        out_shape=outs,
        in_specs=specs,
        out_specs=jax.tree.map(lambda _: pl.BlockSpec(memory_space=pltpu.VMEM), outs),
        compiler_params=pltpu.CompilerParams(vmem_limit_bytes=VLIM),
        cost_estimate=pl.CostEstimate(flops=flops, bytes_accessed=1 << 20, transcendentals=0),
        name=name,
    )(*args)


def shaped(*shape, dtype=F32):
    return jax.ShapeDtypeStruct(shape, dtype)


def ring_pairs(phase, offset):
    pairs = []
    for tp in range(2):
        stride = STRIDES[phase][tp]
        for me in range(64):
            at = (me // stride) % 4
            pairs.append((64 * tp + me, 64 * tp + me - at * stride + ((at + offset) % 4) * stride))
    return pairs


def ring_send(block, phase, offset):
    return lax.ppermute(block, ("tp", "fsdp"), ring_pairs(phase, offset))


ORDER = (2, 1, 3)


def exchange_tables(table, phase):
    rows = table.shape[0] // 4
    blocks = [table[:rows]]
    for o in (1, 2, 3):
        blocks.append(ring_send(table[o * rows:(o + 1) * rows], phase, o))
    return blocks


def exchange_rows(make, phase):
    blocks = {}
    for o in ORDER:
        blocks[o] = ring_send(make(o), phase, o)
    blocks[0] = make(0)
    return [blocks[o] for o in range(4)]


def solution(mesh):
    row_spec = P(("dp", "fsdp"), None)
    act_spec = P(("dp", "fsdp"), None, None)
    table_spec = P(("dp", "tp"), "fsdp")

    def dense_grad(tokens, rows, shard_rows):
        local_ids = tokens - lax.axis_index("tp") * shard_rows
        seg_ids = jnp.where((local_ids >= 0) & (local_ids < shard_rows), local_ids, shard_rows)
        part = jax.ops.segment_sum(rows.astype(F32), seg_ids, num_segments=shard_rows)
        part = part.T.reshape(64, 16, shard_rows)
        got = lax.all_to_all(part, "fsdp", 0, 0, tiled=True)
        return jnp.sum(got, axis=0)

    def local_step(tokens, out_grad, head_grad, master_w, moment_m, moment_v, learn_rate, clip_scale):
        tp, me = lax.axis_index("tp"), lax.axis_index("fsdp")
        x, y, z = me % 4, (me // 4) % 4, me // 16
        low = tp == 0
        coords = jnp.stack([tp, jnp.where(low, x, z), jnp.where(low, y, x), jnp.where(low, z, y)]).astype(I32)
        ids = tokens.reshape(1, -1)
        n = ids.shape[1]
        rows = out_grad.reshape(n, -1)
        width = rows.shape[1] // 2

        slot1, pres1, over1 = call(
            index_first, "index1", (shaped(1, n, dtype=I32), shaped(64, KW), shaped(8, 128)), (coords, ids), 1 << 30, (0,))

        def make1(o):
            depth = 1024
            return pl.pallas_call(
                functools.partial(gather_first, o),
                grid_spec=pltpu.PrefetchScalarGridSpec(
                    num_scalar_prefetch=1,
                    grid=(n // depth,),
                    in_specs=[pl.BlockSpec((1, depth), lambda i, t: (0, i)), pl.BlockSpec((depth, width), lambda i, t: (i, t[0]))],
                    out_specs=pl.BlockSpec((CAP[0], width), lambda i, t: (0, 0)),
                ),
                out_shape=shaped(CAP[0], width),
                compiler_params=pltpu.CompilerParams(vmem_limit_bytes=VLIM),
                cost_estimate=pl.CostEstimate(flops=2 * CAP[0] * n * width, bytes_accessed=n * width * 2, transcendentals=0),
                name=f"gather1_{o}",
            )(coords, slot1, rows)

        def make_next(slots, blocks, cap_out, tag):
            def make(o):
                return call(
                    functools.partial(gather_next, o), f"gather{tag}_{o}", shaped(cap_out, width), (slots, *blocks),
                    2 * cap_out * 12 * blocks[0].shape[0] * width)
            return make

        tables1 = exchange_tables(pres1, 0)
        got1 = exchange_rows(make1, 0)
        slot2, pres2, over2 = call(
            functools.partial(index_next, 4, CAP[0], CAP[1]), "index2",
            (shaped(4, KW, dtype=I32), shaped(16, KW), shaped(8, 128)), (*tables1, over1), 1 << 29)
        pres2 = jnp.repeat(pres2.reshape(4, 4, KW), 2, axis=1).reshape(32, KW)
        tables2 = [t.reshape(4, 2, KW)[:, 0] for t in exchange_tables(pres2, 1)]
        slot3, pres3, over3 = call(
            functools.partial(index_next, 1, CAP[1], CAP[2]), "index3",
            (shaped(4, KW, dtype=I32), shaped(4, KW), shaped(8, 128)), (*tables2, over2), 1 << 29)
        pres3 = jnp.repeat(pres3, 8, axis=0)
        tables3 = exchange_tables(pres3, 2)
        over = jnp.maximum(over3, lax.ppermute(over3, "tp", [(0, 1), (1, 0)]))

        got2 = exchange_rows(make_next(slot2, got1, CAP[1], 2), 1)
        got3 = exchange_rows(make_next(slot3, got2, CAP[2], 3), 2)
        dense = call(dense_last, "dense", shaped(width, KW), (*tables3, *got3, over), 2 * width * KW * 12 * CAP[2])

        lower, upper = dense[:, :256], dense[:, 256:]
        keep = jnp.where(low, lower, upper)
        give = jnp.where(low, upper, lower)
        take = lax.ppermute(give, "tp", [(0, 1), (1, 0)])
        whole = jnp.concatenate([jnp.where(low, keep, take), jnp.where(low, take, keep)], axis=0)
        recv = lax.all_to_all(whole.reshape(64, 16, 256), "fsdp", 0, 0, tiled=True)
        flag = jnp.max(recv[:, 0, 255]) > 0.5

        scal = jnp.stack([learn_rate, clip_scale])
        tables = (head_grad.T, master_w.T, moment_m.T, moment_v.T)
        shard_rows = master_w.shape[0]
        shard = (16, shard_rows)

        def fast(_):
            return pl.pallas_call(
                finish,
                out_shape=(shaped(*shard), shaped(*shard), shaped(*shard), shaped(*shard, dtype=BF16)),
                in_specs=[pl.BlockSpec(memory_space=pltpu.SMEM)] + [pl.BlockSpec(memory_space=pltpu.VMEM)] * 5,
                out_specs=tuple(pl.BlockSpec(memory_space=pltpu.VMEM) for _ in range(4)),
                scratch_shapes=[pltpu.VMEM(((shard_rows + 127) // 128, 16, 128), F32)],
                compiler_params=pltpu.CompilerParams(vmem_limit_bytes=VLIM),
                name="finish",
            )(scal, recv, *tables)

        def slow(_):
            grad = dense_grad(tokens.reshape(-1), rows, shard_rows)
            new_w, new_m, new_v = update_math(grad, *tables, learn_rate, clip_scale)
            return new_w, new_m, new_v, new_w.astype(BF16)

        return tuple(a.T for a in lax.cond(flag, slow, fast, None))

    return jax.shard_map(local_step, mesh=mesh, in_specs=(row_spec, act_spec, table_spec, table_spec, table_spec, table_spec, P(), P()), out_specs=(table_spec, table_spec, table_spec, table_spec), check_vma=False)
```

```python
import functools

import jax
import jax.numpy as jnp
from jax import lax
from jax.experimental import pallas as pl
from jax.experimental.pallas import tpu as pltpu
from jax.sharding import PartitionSpec as P

OPT_STEP = 20
F32, BF16, I32 = jnp.float32, jnp.bfloat16, jnp.int32
CAP = (480, 352, 208)
KW = 512
STRIDES = ((1, 16), (4, 1), (16, 4))
VLIM = 20 << 20
MESH = pl.DeviceIdType.MESH
ORDER = (2, 1, 3, 0)


def update_math(embed_grad, head_grad, master_w, moment_m, moment_v, learn_rate, clip_scale):
    beta_two = 1.0 - OPT_STEP ** -0.8
    grad_full = clip_scale * (embed_grad + head_grad)
    new_v = beta_two * moment_v + (1.0 - beta_two) * (grad_full * grad_full + 1e-30)
    new_m = 0.9 * moment_m + 0.1 * (grad_full / jnp.sqrt(new_v))
    new_w = master_w - learn_rate * new_m - learn_rate * learn_rate * master_w
    return new_w, new_m, new_v


def iota(shape, dim):
    return lax.broadcasted_iota(I32, shape, dim)


def onehot(cond):
    return jnp.where(cond, 1.0, 0.0).astype(BF16)


def dot_nt(a, b):
    return lax.dot_general(a, b, (((1,), (1,)), ((), ())), preferred_element_type=F32)


def dot_nn(a, b):
    return jnp.dot(a, b, preferred_element_type=F32)


def ranks(pres, group):
    rows = pres.shape[0]
    pres_b = pres.astype(BF16)
    before = onehot(iota((KW, KW), 0) < iota((KW, KW), 1))
    inner = dot_nn(pres_b, before)
    if group > 1:
        r, c = iota((rows, rows), 0), iota((rows, rows), 1)
        above = onehot((c < r) & (c // group == r // group))
        inner = inner + jnp.sum(dot_nn(above, pres_b), axis=1, keepdims=True)
    return inner.astype(I32)


def codes(pres, group, cap):
    rows = pres.shape[0]
    rank = ranks(pres, group)
    code = jnp.where((pres > 0.5) & (rank < cap), (iota((rows, KW), 0) // group) * cap + rank + 1, 0)
    over = jnp.where((pres > 0.5) & (rank >= cap), 1.0, 0.0)
    return code, jnp.max(over)


def index_first(coords, tok_ref, slot_ref, tables):
    ids = tok_ref[...]
    tp, c1, c2, c3 = coords
    x, y, z = ids & 3, (ids >> 2) & 3, (ids >> 4) & 3
    d1 = x + (z - x) * tp
    d2 = y + (x - y) * tp
    d3 = z + (y - z) * tp
    q = (((d1 - c1) & 3) << 4) + (((d2 - c2) & 3) << 2) + ((d3 - c3) & 3)
    upper = ids >= 16064
    kk = jnp.where(upper, ids - 16064, ids) >> 6
    k = jnp.where(upper, 256, 0) + ((kk & 1) << 7) + (kk >> 1)
    n = ids.shape[1]
    hot_q = onehot(iota((64, n), 0) == q)
    hot_k = onehot(iota((KW, n), 0) == k)
    pres = jnp.minimum(dot_nt(hot_q, hot_k), 1.0)
    code, over = codes(pres, 16, CAP[0])
    both = jnp.concatenate([(code >> 5).astype(BF16), (code & 31).astype(BF16)], axis=0)
    found = dot_nn(both, hot_k)
    value = found[:64] * 32.0 + found[64:]
    slot_ref[...] = jnp.sum(jnp.where(iota((64, n), 0) == q, value, 0.0), axis=0, keepdims=True).astype(I32) - 1
    for o in range(4):
        tables[o] = pres[16 * o:16 * o + 16]
    return over


def gather_first(o, slot_ref, rows_ref, out_ref):
    cap, depth = out_ref.shape[0], 1024

    def step(n, first):
        at = pl.ds(pl.multiple_of(n * depth, depth), depth)
        hot = onehot(iota((cap, depth), 0) == slot_ref[:, at] - o * cap)
        part = dot_nn(hot, rows_ref[at, :])
        out_ref[...] = part if first else out_ref[...] + part

    step(0, True)
    lax.fori_loop(1, rows_ref.shape[0] // depth, lambda n, c: (step(n, False), c)[1], 0)


def index_next(group, cap_out, blocks, slot_ref, tables):
    blocks = [block[:4 * group] for block in blocks]
    merged = jnp.minimum(blocks[0] + blocks[1] + blocks[2] + blocks[3], 1.0)
    rows = merged.shape[0]
    code, over = codes(merged, group, cap_out)
    hi, lo = (code >> 5).astype(F32), (code & 31).astype(F32)
    lanes = iota((32, KW), 1)
    spread = onehot((lanes & 31) == iota((32, KW), 0))
    own_row = (iota((16, KW), 1) >> 5) == iota((16, KW), 0)
    for s, pres in enumerate(blocks):
        rank = jnp.where(pres > 0.5, ranks(pres, rows), -1)
        table = jnp.zeros((16, 64), F32)
        for r in range(rows):
            row = rank[r:r + 1]
            high = onehot(iota((16, KW), 0) == (row >> 5))
            low = iota((32, KW), 0) == (row & 31)
            low = jnp.concatenate([jnp.where(low, hi[r:r + 1], 0.0), jnp.where(low, lo[r:r + 1], 0.0)], axis=0)
            table = table + dot_nt(high, low.astype(BF16))
        table = table.astype(BF16)
        value = dot_nn(table[:, :32], spread) * 32.0 + dot_nn(table[:, 32:], spread)
        slot_ref[s:s + 1, :] = jnp.sum(jnp.where(own_row, value, 0.0), axis=0, keepdims=True).astype(I32) - 1
    tables[...] = jnp.zeros(tables.shape, F32)
    for o in range(4):
        tables[o, :group] = merged[group * o:group * o + group]
    return over


def split_rows(rows):
    high = jnp.clip(rows, -3.38e38, 3.38e38).astype(BF16)
    rest = rows - high.astype(F32)
    mid = rest.astype(BF16)
    return high, mid, (rest - mid.astype(F32)).astype(BF16)


def gather_next(o, slot_ref, blocks, out_ref):
    cap_out, cap_in = out_ref.shape[0], blocks[0].shape[0]
    hots = [onehot(iota((cap_out, cap_in), 0) == slot_ref[s:s + 1, :cap_in] - o * cap_out) for s in range(4)]

    def columns(n, carry):
        at = pl.ds(pl.multiple_of(n * 256, 256), 256)
        total = None
        for hot, rows in zip(hots, blocks):
            for piece in split_rows(rows[:, at]):
                part = dot_nn(hot, piece)
                total = part if total is None else total + part
        out_ref[:, at] = total
        return carry

    lax.fori_loop(0, out_ref.shape[1] // 256, columns, 0)


def dense_last(tables, blocks, flag, out_ref):
    total = None
    for pres_ref, rows in zip(tables, blocks):
        pres = pres_ref[...]
        rank = jnp.where(pres > 0.5, ranks(pres, 1), -1)[0:1]
        hot = onehot(iota((rows.shape[0], KW), 0) == rank)
        for piece in split_rows(rows[...].T):
            part = dot_nn(piece, hot)
            total = part if total is None else total + part
    total = jnp.where((iota(total.shape, 1) & 255) == 255, flag, total)
    for t in range(2):
        out_ref[t] = total[:, 256 * t:256 * t + 256].reshape(out_ref.shape[1:])


def assemble(tok_ref, rows_ref, recv_ref, half, slot1, slot2, slot3, tab1, tab2, tab3, rtab1, rtab2, rtab3, send1, send2, send3,
             recv1, recv2, recv3, own_over, peer_over, dense, half_sem, tab_out, tab_in, row_out, row_in, over_out, over_in, last_out, last_in):
    tp, me = lax.axis_index("tp"), lax.axis_index("fsdp")
    ring = []
    for low, high in STRIDES:
        stride = low + (high - low) * tp
        ring.append((stride, (me // stride) % 4))
    coords = (tp, *(at for _, at in ring))
    width = half.shape[1]
    side = me // 32
    same = 1 - (side + tp) % 2

    def neighbour(phase, offset):
        stride, at = ring[phase]
        return {"fsdp": me + stride * ((at + offset) % 4 - at)}

    barrier = pltpu.get_barrier_semaphore()

    def greet(device):
        pl.semaphore_signal(barrier, inc=1, device_id=device, device_id_type=MESH)

    for phase in range(3):
        for o in (1, 2, 3):
            greet(neighbour(phase, o))
    greet({"tp": 1 - tp})

    def greet_source(i, carry):
        greet({"fsdp": (me + i) % 64, "tp": side})
        return carry

    lax.fori_loop(1, 64, greet_source, 0)

    @pl.when(same == 0)
    def _():
        greet({"tp": side})

    load = pltpu.make_async_copy(rows_ref.at[:, pl.ds(pl.multiple_of(tp * width, width), width)], half, half_sem)
    load.start()
    over = index_first(coords, tok_ref, slot1, tab1)
    pl.semaphore_wait(barrier, 74 - same)

    def remote(src, dst, out, into, device):
        copy = pltpu.make_async_remote_copy(
            src_ref=src, dst_ref=dst, send_sem=out, recv_sem=into, device_id=device, device_id_type=MESH)
        copy.start()
        return copy

    def send_tables(phase, table, into):
        return [remote(table.at[o], into.at[o - 1], tab_out.at[3 * phase + o - 1], tab_in.at[3 * phase + o - 1], neighbour(phase, o))
                for o in (1, 2, 3)]

    def send_row(phase, o, rows, into):
        return remote(rows.at[o], into.at[o - 1], row_out.at[3 * phase + o - 1], row_in.at[3 * phase + o - 1], neighbour(phase, o))

    def wait(copies):
        for copy in copies:
            copy.wait()

    def beside(own, got):
        return [own.at[0], *(got.at[n] for n in range(3))]

    tables = send_tables(0, tab1, rtab1)
    load.wait()
    rows = []
    for o in ORDER:
        gather_first(o, slot1, half, send1.at[o])
        if o:
            rows.append(send_row(0, o, send1, recv1))

    wait(tables)
    over = jnp.maximum(over, index_next(4, CAP[1], beside(tab1, rtab1), slot2, tab2))
    tables = send_tables(1, tab2, rtab2)
    wait(tables)
    over = jnp.maximum(over, index_next(1, CAP[2], beside(tab2, rtab2), slot3, tab3))
    own_over[...] = jnp.full(own_over.shape, over, F32)
    tables = send_tables(2, tab3, rtab3)
    tables.append(remote(own_over, peer_over, over_out, over_in, {"tp": 1 - tp}))

    wait(rows)
    rows = []
    for o in ORDER:
        gather_next(o, slot2, beside(send1, recv1), send2.at[o])
        if o:
            rows.append(send_row(1, o, send2, recv2))
    wait(rows)
    rows = []
    for o in ORDER:
        gather_next(o, slot3, beside(send2, recv2), send3.at[o])
        if o:
            rows.append(send_row(2, o, send3, recv3))
    wait(tables)
    wait(rows)
    flag = jnp.maximum(own_over[0:1, 0:1], peer_over[0:1, 0:1])
    dense_last(beside(tab3, rtab3), beside(send3, recv3), flag, dense)

    def last(i, far):
        at = (me + i) % 32
        core = (tp + far) % 2
        return pltpu.make_async_remote_copy(
            src_ref=dense.at[core, at], dst_ref=recv_ref.at[me], send_sem=last_out.at[2 * i + far], recv_sem=last_in.at[me],
            device_id={"fsdp": 32 * tp + at, "tp": core}, device_id_type=MESH)

    def arrive(j):
        return pltpu.make_async_remote_copy(
            src_ref=dense.at[0, 0], dst_ref=recv_ref.at[j], send_sem=last_out.at[0], recv_sem=last_in.at[j],
            device_id={"tp": 1 - tp}, device_id_type=MESH)

    def start_pair(i, carry):
        last(i, 0).start()
        last(i, 1).start()
        return carry

    lax.fori_loop(1, 32, start_pair, 0)
    last(0, 1).start()

    @pl.when(same == 0)
    def _():
        last(0, 0).start()

    @pl.when(same == 1)
    def _():
        recv_ref[me] = dense[tp, me % 32]

    def wait_pair(i, carry):
        last(i, 0).wait_send()
        last(i, 1).wait_send()
        return carry

    def wait_arrival(i, carry):
        arrive((me + i) % 64).wait_recv()
        return carry

    lax.fori_loop(1, 64, wait_arrival, 0)
    lax.fori_loop(1, 32, wait_pair, 0)
    last(0, 1).wait_send()

    @pl.when(same == 0)
    def _():
        arrive(me).wait_recv()
        last(0, 0).wait_send()


def finish(scal_ref, recv_ref, head_ref, w_ref, m_ref, v_ref, w_out, m_out, v_out, b_out, grad):
    tiles = grad.shape[0]
    for c in range(16):
        both = jnp.concatenate([recv_ref[:, c, :128], recv_ref[:, c, 128:]], axis=0)
        grad[:, c, :] = both.T[:tiles]
    lr, clip = scal_ref[0], scal_ref[1]
    rows = head_ref.shape[1]
    for t in range(tiles):
        at = slice(128 * t, min(128 * t + 128, rows))
        width = at.stop - at.start
        new_w, new_m, new_v = update_math(grad[t, :, :width], head_ref[:, at], w_ref[:, at], m_ref[:, at], v_ref[:, at], lr, clip)
        w_out[:, at], m_out[:, at], v_out[:, at] = new_w, new_m, new_v
        b_out[:, at] = new_w.astype(BF16)


def shaped(*shape, dtype=F32):
    return jax.ShapeDtypeStruct(shape, dtype)


def dense_rows(ids_ref, rows_ref, out_ref):
    first = pl.program_id(0) * out_ref.shape[0]
    hot = onehot(iota((out_ref.shape[0], rows_ref.shape[0]), 0) + first == ids_ref[...])
    part = dot_nn(hot, rows_ref[...])

    @pl.when(pl.program_id(1) == 0)
    def _():
        out_ref[...] = part

    @pl.when(pl.program_id(1) > 0)
    def _():
        out_ref[...] += part


def solution(mesh):
    row_spec = P(("dp", "fsdp"), None)
    act_spec = P(("dp", "fsdp"), None, None)
    table_spec = P(("dp", "tp"), "fsdp")

    def dense_grad(ids, rows, shard_rows):
        n, width = rows.shape
        block, depth = 256, 1024
        tiles = -(-shard_rows // block)
        part = pl.pallas_call(
            dense_rows,
            grid=(tiles, n // depth),
            in_specs=[pl.BlockSpec((1, depth), lambda i, k: (0, k)), pl.BlockSpec((depth, width), lambda i, k: (k, 0))],
            out_specs=pl.BlockSpec((block, width), lambda i, k: (i, 0)),
            out_shape=shaped(tiles * block, width),
            compiler_params=pltpu.CompilerParams(vmem_limit_bytes=VLIM),
            name="dense_rows",
        )(ids - lax.axis_index("tp") * shard_rows, rows)
        part = part[:shard_rows].T.reshape(64, 16, shard_rows)
        return jnp.sum(lax.all_to_all(part, "fsdp", 0, 0, tiled=True), axis=0)

    def local_step(tokens, out_grad, head_grad, master_w, moment_m, moment_v, learn_rate, clip_scale):
        ids = tokens.reshape(1, -1)
        n = ids.shape[1]
        rows = out_grad.reshape(n, -1)
        width = rows.shape[1] // 2
        vm, dma = pltpu.VMEM, pltpu.SemaphoreType.DMA
        recv = pl.pallas_call(
            assemble,
            out_shape=shaped(64, 16, 256),
            in_specs=[pl.BlockSpec(memory_space=vm), pl.BlockSpec(memory_space=pl.ANY)],
            out_specs=pl.BlockSpec(memory_space=vm),
            scratch_shapes=[
                vm((n, width), BF16), vm((1, n), I32), vm((4, KW), I32), vm((4, KW), I32),
                vm((4, 16, KW), F32), vm((4, 8, KW), F32), vm((4, 8, KW), F32),
                vm((3, 16, KW), F32), vm((3, 8, KW), F32), vm((3, 8, KW), F32),
                *[vm((4, cap, width), F32) for cap in CAP],
                *[vm((3, cap, width), F32) for cap in CAP],
                vm((8, 128), F32), vm((8, 128), F32), vm((2, 32, 16, 256), F32),
                dma, dma((9,)), dma((9,)), dma((9,)), dma((9,)), dma, dma, dma((64,)), dma((64,)),
            ],
            compiler_params=pltpu.CompilerParams(vmem_limit_bytes=52 << 20, collective_id=0, has_side_effects=True),
            name="assemble",
        )(ids, rows)
        flag = jnp.max(recv[:, 0, 255]) > 0.5

        scal = jnp.stack([learn_rate, clip_scale])
        tables = (head_grad.T, master_w.T, moment_m.T, moment_v.T)
        shard_rows = master_w.shape[0]
        shard = (16, shard_rows)

        def fast(_):
            return pl.pallas_call(
                finish,
                out_shape=(shaped(*shard), shaped(*shard), shaped(*shard), shaped(*shard, dtype=BF16)),
                in_specs=[pl.BlockSpec(memory_space=pltpu.SMEM)] + [pl.BlockSpec(memory_space=pltpu.VMEM)] * 5,
                out_specs=tuple(pl.BlockSpec(memory_space=pltpu.VMEM) for _ in range(4)),
                scratch_shapes=[pltpu.VMEM(((shard_rows + 127) // 128, 16, 128), F32)],
                compiler_params=pltpu.CompilerParams(vmem_limit_bytes=VLIM),
                name="finish",
            )(scal, recv, *tables)

        def slow(_):
            grad = dense_grad(ids, rows, shard_rows)
            new_w, new_m, new_v = update_math(grad, *tables, learn_rate, clip_scale)
            return new_w, new_m, new_v, new_w.astype(BF16)

        return tuple(a.T for a in lax.cond(flag, slow, fast, None))

    return jax.shard_map(local_step, mesh=mesh, in_specs=(row_spec, act_spec, table_spec, table_spec, table_spec, table_spec, P(), P()), out_specs=(table_spec, table_spec, table_spec, table_spec), check_vma=False)
```

```python
import functools

import jax
import jax.numpy as jnp
from jax import lax
from jax.experimental import pallas as pl
from jax.experimental.pallas import tpu as pltpu
from jax.sharding import PartitionSpec as P

OPT_STEP = 20
F32, BF16, I32, I16 = jnp.float32, jnp.bfloat16, jnp.int32, jnp.int16
CAP = (480, 352, 208)
KW = 512
STRIDES = ((1, 16), (4, 1), (16, 4))
VLIM = 20 << 20
MESH = pl.DeviceIdType.MESH
CHUNK = 256


def update_math(embed_grad, head_grad, master_w, moment_m, moment_v, learn_rate, clip_scale):
    beta_two = 1.0 - OPT_STEP ** -0.8
    grad_full = clip_scale * (embed_grad + head_grad)
    new_v = beta_two * moment_v + (1.0 - beta_two) * (grad_full * grad_full + 1e-30)
    new_m = 0.9 * moment_m + 0.1 * (grad_full / jnp.sqrt(new_v))
    new_w = master_w - learn_rate * new_m - learn_rate * learn_rate * master_w
    return new_w, new_m, new_v


def iota(shape, dim):
    return lax.broadcasted_iota(I32, shape, dim)


def onehot(cond):
    return jnp.where(cond, 1.0, 0.0).astype(BF16)


def slots_hot(slots, first, cap):
    row = (slots - first).astype(I16)
    return jnp.where(lax.broadcasted_iota(I16, (cap, slots.shape[1]), 0) == row, BF16(1), BF16(0))


def dot_nt(a, b):
    return lax.dot_general(a, b, (((1,), (1,)), ((), ())), preferred_element_type=F32)


def dot_nn(a, b):
    return jnp.dot(a, b, preferred_element_type=F32)


def ranks(pres, group):
    rows = pres.shape[0]
    pres_b = pres.astype(BF16)
    before = onehot(iota((KW, KW), 0) < iota((KW, KW), 1))
    inner = dot_nn(pres_b, before)
    if group > 1:
        r, c = iota((rows, rows), 0), iota((rows, rows), 1)
        above = onehot((c < r) & (c // group == r // group))
        inner = inner + jnp.sum(dot_nn(above, pres_b), axis=1, keepdims=True)
    return inner.astype(I32)


def codes(pres, group, cap):
    rows = pres.shape[0]
    rank = ranks(pres, group)
    code = jnp.where((pres > 0.5) & (rank < cap), (iota((rows, KW), 0) // group) * cap + rank + 1, 0)
    over = jnp.where((pres > 0.5) & (rank >= cap), 1.0, 0.0)
    return code, jnp.max(over)


def index_first(coords, tok_ref, slot_ref, tables):
    ids = jnp.concatenate([tok_ref[r:r + 1] for r in range(tok_ref.shape[0])], axis=1)
    tp, c1, c2, c3 = coords
    x, y, z = ids & 3, (ids >> 2) & 3, (ids >> 4) & 3
    d1 = x + (z - x) * tp
    d2 = y + (x - y) * tp
    d3 = z + (y - z) * tp
    q = (((d1 - c1) & 3) << 4) + (((d2 - c2) & 3) << 2) + ((d3 - c3) & 3)
    upper = ids >= 16064
    kk = jnp.where(upper, ids - 16064, ids) >> 6
    k = jnp.where(upper, 256, 0) + ((kk & 1) << 7) + (kk >> 1)
    n = ids.shape[1]
    hot_q = onehot(iota((64, n), 0) == q)
    hot_k = onehot(iota((KW, n), 0) == k)
    pres = jnp.minimum(dot_nt(hot_q, hot_k), 1.0)
    code, over = codes(pres, 16, CAP[0])
    both = jnp.concatenate([(code >> 5).astype(BF16), (code & 31).astype(BF16)], axis=0)
    found = dot_nn(both, hot_k)
    value = found[:64] * 32.0 + found[64:]
    slot_ref[...] = jnp.sum(jnp.where(iota((64, n), 0) == q, value, 0.0), axis=0, keepdims=True).astype(I32) - 1
    for o in range(4):
        tables[o] = pres[16 * o:16 * o + 16]
    return over


def gather_first(o, slot_ref, rows_ref, outs):
    cap, depth = outs[0].shape[0], 1024

    def step(n, first):
        at = pl.ds(pl.multiple_of(n * depth, depth), depth)
        part = dot_nn(slots_hot(slot_ref[:, at], o * cap, cap), rows_ref[at, :])
        for chunk, out in enumerate(outs):
            piece = part[:, CHUNK * chunk:CHUNK * chunk + CHUNK]
            out[...] = piece if first else out[...] + piece

    step(0, True)
    lax.fori_loop(1, rows_ref.shape[0] // depth, lambda n, c: (step(n, False), c)[1], 0)


def index_next(group, cap_in, cap_out, blocks, slot_ref, tables):
    rows = 4 * group
    blocks = [block[:rows] for block in blocks]
    merged = jnp.minimum(blocks[0] + blocks[1] + blocks[2] + blocks[3], 1.0)
    code, over = codes(merged, group, cap_out)
    hi, lo = (code >> 5).astype(F32), (code & 31).astype(F32)
    every = jnp.concatenate(blocks, axis=0)
    every = jnp.where(every > 0.5, ranks(every, rows), -1)
    spread = onehot((iota((16, KW), 1) >> 5) == iota((16, KW), 0))
    own_row = (iota((32, KW), 1) & 31) == iota((32, KW), 0)
    found = []
    for s in range(4):
        highs, lows = [], []
        for r in range(rows):
            row = every[rows * s + r:rows * s + r + 1]
            highs.append(onehot(iota((16, KW), 0) == (row >> 5)))
            low = iota((32, KW), 0) == (row & 31)
            low = jnp.concatenate([jnp.where(low, hi[r:r + 1], 0.0), jnp.where(low, lo[r:r + 1], 0.0)], axis=0)
            lows.append(low.astype(BF16))
        table = dot_nt(jnp.concatenate(lows, axis=1), jnp.concatenate(highs, axis=1)).astype(BF16)
        value = dot_nn(table, spread)
        value = jnp.where(own_row, value[:32] * 32.0 + value[32:], 0.0)
        found.append(jnp.sum(value, axis=0, keepdims=True)[:, :cap_in])
    slot_ref[:, :4 * cap_in] = jnp.concatenate(found, axis=1).astype(I32) - 1
    tables[...] = jnp.zeros(tables.shape, F32)
    for o in range(4):
        tables[o, :group] = merged[group * o:group * o + group]
    return over


def split_rows(rows):
    high = jnp.clip(rows, -3.38e38, 3.38e38).astype(BF16)
    rest = rows - high.astype(F32)
    mid = rest.astype(BF16)
    return high, mid, (rest - mid.astype(F32)).astype(BF16)


def split_blocks(blocks, pieces):
    cap = blocks[0].shape[0]
    for s, rows in enumerate(blocks):
        for n, piece in enumerate(split_rows(rows[...])):
            pieces[n, cap * s:cap * s + cap] = piece


def gather_next(o, depth, slot_ref, pieces, out_ref):
    cap = out_ref.shape[0]
    hot = slots_hot(slot_ref[:, :depth], o * cap, cap)
    out_ref[...] = dot_nn(hot, pieces[0, :depth]) + dot_nn(hot, pieces[1, :depth]) + dot_nn(hot, pieces[2, :depth])


def dense_last(tables, blocks, flag, out_ref):
    pres = jnp.concatenate([table[...] for table in tables], axis=0)
    rank = jnp.where(pres > 0.5, ranks(pres, 1), -1)
    cap = blocks[0].shape[0]
    hot = jnp.concatenate([slots_hot(rank[8 * s:8 * s + 1], 0, cap) for s in range(4)], axis=0)
    rows = jnp.concatenate([block[...] for block in blocks], axis=0).T
    high, mid, low = split_rows(rows)
    total = dot_nn(high, hot) + dot_nn(mid, hot) + dot_nn(low, hot)
    total = jnp.where((iota(total.shape, 1) & 255) == 255, flag, total)
    for t in range(2):
        out_ref[t] = total[:, 256 * t:256 * t + 256].reshape(out_ref.shape[1:])


def assemble(tok_ref, rows_ref, recv_ref, half, slot1, slot2, slot3, tab1, tab2, tab3, rtab1, rtab2, rtab3, send1, send2, send3,
             recv1, recv2, recv3, pieces, own_over, peer_over, dense, half_sem, tab_out, tab_in, row_out, row_in, over_out, over_in, last_out, last_in):
    tp, me = lax.axis_index("tp"), lax.axis_index("fsdp")
    ring = []
    for low, high in STRIDES:
        stride = low + (high - low) * tp
        ring.append((stride, (me // stride) % 4))
    coords = (tp, *(at for _, at in ring))
    width = half.shape[1]
    same = 1 - (me // 32 + tp) % 2

    def neighbour(phase, offset):
        stride, at = ring[phase]
        return {"fsdp": me + stride * ((at + offset) % 4 - at)}

    barrier = pltpu.get_barrier_semaphore()

    def greet(device):
        pl.semaphore_signal(barrier, inc=1, device_id=device, device_id_type=MESH)

    for phase in range(3):
        for o in (1, 2, 3):
            greet(neighbour(phase, o))
    greet({"tp": 1 - tp})

    load = pltpu.make_async_copy(rows_ref.at[:, pl.ds(pl.multiple_of(tp * width, width), width)], half, half_sem)
    load.start()
    over = index_first(coords, tok_ref, slot1, tab1)
    pl.semaphore_wait(barrier, 10)

    def copy_to(src, dst, out, into, device):
        return pltpu.make_async_remote_copy(
            src_ref=src, dst_ref=dst, send_sem=out, recv_sem=into, device_id=device, device_id_type=MESH)

    def remote(*args):
        copy = copy_to(*args)
        copy.start()
        return copy

    def send_tables(phase, table, into):
        return [remote(table.at[o], into.at[o - 1], tab_out.at[3 * phase + o - 1], tab_in.at[3 * phase + o - 1], neighbour(phase, o))
                for o in (1, 2, 3)]

    def send_row(phase, chunk, o, rows, into):
        sem = 6 * phase + 3 * chunk + o - 1
        return copy_to(rows.at[chunk, o], into.at[chunk, o - 1], row_out.at[sem], row_in.at[sem], neighbour(phase, o))

    def wait(copies):
        for copy in copies:
            copy.wait()

    def beside(own, got):
        return [own.at[0], *(got.at[n] for n in range(3))]

    def loop_bins(step):
        lax.fori_loop(0, 3, lambda n, c: (step(2 - n + 3 * (n // 2)), c)[1], 0)

    def first(o):
        gather_first(o, slot1, half, [send1.at[chunk, o] for chunk in range(2)])

    def first_sent(o):
        first(o)
        send_row(0, 0, o, send1, recv1).start()

    def later(phase, chunk):
        slot, own, got, out, into = ((slot2, send1, recv1, send2, recv2), (slot3, send2, recv2, send3, recv3))[phase - 1]
        blocks = beside(own.at[chunk], got.at[chunk])
        depth = 4 * CAP[phase - 1]
        split_blocks(blocks, pieces)

        def sent(o):
            gather_next(o, depth, slot, pieces, out.at[chunk, o])
            send_row(phase, chunk, o, out, into).start()

        loop_bins(sent)
        gather_next(0, depth, slot, pieces, out.at[chunk, 0])

    def wait_rows(phase, chunk):
        out, into = ((send1, recv1), (send2, recv2), (send3, recv3))[phase]
        for o in (1, 2, 3):
            send_row(phase, chunk, o, out, into).wait()

    def finish_chunk(chunk):
        dense_last(beside(tab3, rtab3), beside(send3.at[chunk], recv3.at[chunk]), flag, dense.at[chunk])

    tables1 = send_tables(0, tab1, rtab1)
    load.wait()
    loop_bins(first_sent)
    for o in (2, 1, 3):
        send_row(0, 1, o, send1, recv1).start()
    wait(tables1)
    over = jnp.maximum(over, index_next(4, CAP[0], CAP[1], beside(tab1, rtab1), slot2, tab2))
    tables2 = send_tables(1, tab2, rtab2)
    first(0)
    wait(tables2)
    over = jnp.maximum(over, index_next(1, CAP[1], CAP[2], beside(tab2, rtab2), slot3, tab3))
    own_over[...] = jnp.full(own_over.shape, over, F32)
    tables3 = send_tables(2, tab3, rtab3)
    tables3.append(remote(own_over, peer_over, over_out, over_in, {"tp": 1 - tp}))
    wait_rows(0, 0)

    @pl.when(tp == 1)
    def _():
        wait_rows(0, 1)

    later(1, 0)

    @pl.when(tp == 0)
    def _():
        wait_rows(0, 1)

    later(1, 1)
    wait_rows(1, 0)
    later(2, 0)
    wait(tables3)
    flag = jnp.maximum(own_over[0:1, 0:1], peer_over[0:1, 0:1])
    wait_rows(1, 1)
    later(2, 1)
    wait_rows(2, 0)
    finish_chunk(0)

    def last(i, far):
        at = (me + i) % 32
        core = (tp + far) % 2
        return pltpu.make_async_remote_copy(
            src_ref=dense.at[at // 16, core, at % 16], dst_ref=recv_ref.at[me], send_sem=last_out.at[2 * i + far],
            recv_sem=last_in.at[me], device_id={"fsdp": 32 * tp + at, "tp": core}, device_id_type=MESH)

    def arrive(j):
        return pltpu.make_async_remote_copy(
            src_ref=dense.at[0, 0, 0], dst_ref=recv_ref.at[j], send_sem=last_out.at[0], recv_sem=last_in.at[j],
            device_id={"tp": 1 - tp}, device_id_type=MESH)

    def each_pair(chunk, act, self_act):
        def pair(n, carry):
            at = 16 * chunk + (me + n) % 16
            i = (at - me % 32 + 32) % 32
            act(last(i, 1))

            @pl.when((same == 0) | (i > 0))
            def _():
                act(last(i, 0))

            @pl.when((same == 1) & (i == 0))
            def _():
                self_act()

            return carry

        lax.fori_loop(0, 16, pair, 0)

    def keep():
        recv_ref[me] = dense[(me % 32) // 16, tp, me % 16]

    each_pair(0, lambda copy: copy.start(), keep)
    wait_rows(2, 1)
    finish_chunk(1)
    each_pair(1, lambda copy: copy.start(), keep)

    def wait_arrival(i, carry):
        arrive((me + i) % 64).wait_recv()
        return carry

    lax.fori_loop(1, 64, wait_arrival, 0)

    @pl.when(same == 0)
    def _():
        arrive(me).wait_recv()

    each_pair(0, lambda copy: copy.wait_send(), lambda: None)
    each_pair(1, lambda copy: copy.wait_send(), lambda: None)


def finish(scal_ref, recv_ref, head_ref, w_ref, m_ref, v_ref, w_out, m_out, v_out, b_out, grad):
    tiles = grad.shape[0]
    for c in range(16):
        both = jnp.concatenate([recv_ref[:, c, :128], recv_ref[:, c, 128:]], axis=0)
        grad[:, c, :] = both.T[:tiles]
    lr, clip = scal_ref[0], scal_ref[1]
    rows = head_ref.shape[1]
    for t in range(tiles):
        at = slice(128 * t, min(128 * t + 128, rows))
        width = at.stop - at.start
        new_w, new_m, new_v = update_math(grad[t, :, :width], head_ref[:, at], w_ref[:, at], m_ref[:, at], v_ref[:, at], lr, clip)
        w_out[:, at], m_out[:, at], v_out[:, at] = new_w, new_m, new_v
        b_out[:, at] = new_w.astype(BF16)


def shaped(*shape, dtype=F32):
    return jax.ShapeDtypeStruct(shape, dtype)


def dense_rows(ids_ref, rows_ref, out_ref):
    first = pl.program_id(0) * out_ref.shape[0]
    hot = onehot(iota((out_ref.shape[0], rows_ref.shape[0]), 0) + first == ids_ref[...])
    part = dot_nn(hot, rows_ref[...])

    @pl.when(pl.program_id(1) == 0)
    def _():
        out_ref[...] = part

    @pl.when(pl.program_id(1) > 0)
    def _():
        out_ref[...] += part


def solution(mesh):
    row_spec = P(("dp", "fsdp"), None)
    act_spec = P(("dp", "fsdp"), None, None)
    table_spec = P(("dp", "tp"), "fsdp")

    def dense_grad(ids, rows, shard_rows):
        n, width = rows.shape
        block, depth = 256, 1024
        tiles = -(-shard_rows // block)
        part = pl.pallas_call(
            dense_rows,
            grid=(tiles, n // depth),
            in_specs=[pl.BlockSpec((1, depth), lambda i, k: (0, k)), pl.BlockSpec((depth, width), lambda i, k: (k, 0))],
            out_specs=pl.BlockSpec((block, width), lambda i, k: (i, 0)),
            out_shape=shaped(tiles * block, width),
            compiler_params=pltpu.CompilerParams(vmem_limit_bytes=VLIM),
            name="dense_rows",
        )(ids - lax.axis_index("tp") * shard_rows, rows)
        part = part[:shard_rows].T.reshape(64, 16, shard_rows)
        return jnp.sum(lax.all_to_all(part, "fsdp", 0, 0, tiled=True), axis=0)

    def local_step(tokens, out_grad, head_grad, master_w, moment_m, moment_v, learn_rate, clip_scale):
        n = tokens.size
        rows = out_grad.reshape(n, -1)
        width = rows.shape[1] // 2
        vm, dma = pltpu.VMEM, pltpu.SemaphoreType.DMA
        recv = pl.pallas_call(
            assemble,
            out_shape=shaped(64, 16, 256),
            in_specs=[pl.BlockSpec(memory_space=vm), pl.BlockSpec(memory_space=pl.ANY)],
            out_specs=pl.BlockSpec(memory_space=vm),
            scratch_shapes=[
                vm((n, width), BF16), vm((1, n), I32), vm((1, 4 * KW), I32), vm((1, 4 * KW), I32),
                vm((4, 16, KW), F32), vm((4, 8, KW), F32), vm((4, 8, KW), F32),
                vm((3, 16, KW), F32), vm((3, 8, KW), F32), vm((3, 8, KW), F32),
                *[vm((2, 4, cap, CHUNK), F32) for cap in CAP],
                *[vm((2, 3, cap, CHUNK), F32) for cap in CAP],
                vm((3, 4 * CAP[0], CHUNK), BF16),
                vm((8, 128), F32), vm((8, 128), F32), vm((2, 2, 16, 16, 256), F32),
                dma, dma((9,)), dma((9,)), dma((18,)), dma((18,)), dma, dma, dma((64,)), dma((64,)),
            ],
            compiler_params=pltpu.CompilerParams(vmem_limit_bytes=40 << 20, collective_id=0, has_side_effects=True),
            name="assemble",
        )(tokens, rows)
        flag = jnp.max(recv[:, 0, 255]) > 0.5

        scal = jnp.stack([learn_rate, clip_scale])
        tables = (head_grad.T, master_w.T, moment_m.T, moment_v.T)
        shard_rows = master_w.shape[0]
        shard = (16, shard_rows)

        def fast(_):
            return pl.pallas_call(
                finish,
                out_shape=(shaped(*shard), shaped(*shard), shaped(*shard), shaped(*shard, dtype=BF16)),
                in_specs=[pl.BlockSpec(memory_space=pltpu.SMEM)] + [pl.BlockSpec(memory_space=pltpu.VMEM)] * 5,
                out_specs=tuple(pl.BlockSpec(memory_space=pltpu.VMEM) for _ in range(4)),
                scratch_shapes=[pltpu.VMEM(((shard_rows + 127) // 128, 16, 128), F32)],
                compiler_params=pltpu.CompilerParams(vmem_limit_bytes=VLIM),
                name="finish",
            )(scal, recv, *tables)

        def slow(_):
            grad = dense_grad(tokens.reshape(1, -1), rows, shard_rows)
            new_w, new_m, new_v = update_math(grad, *tables, learn_rate, clip_scale)
            return new_w, new_m, new_v, new_w.astype(BF16)

        return tuple(a.T for a in lax.cond(flag, slow, fast, None))

    return jax.shard_map(local_step, mesh=mesh, in_specs=(row_spec, act_spec, table_spec, table_spec, table_spec, table_spec, P(), P()), out_specs=(table_spec, table_spec, table_spec, table_spec), check_vma=False)
```

```python
import functools

import jax
import jax.numpy as jnp
from jax import lax
from jax.experimental import pallas as pl
from jax.experimental.pallas import tpu as pltpu
from jax.sharding import PartitionSpec as P

OPT_STEP = 20
F32, BF16, I32, I16 = jnp.float32, jnp.bfloat16, jnp.int32, jnp.int16
CAP = (480, 352, 208)
KW = 512
STRIDES = ((1, 16), (4, 1), (16, 4))
VLIM = 20 << 20
MESH = pl.DeviceIdType.MESH
CHUNK = 256


def update_math(embed_grad, head_grad, master_w, moment_m, moment_v, learn_rate, clip_scale):
    beta_two = 1.0 - OPT_STEP ** -0.8
    grad_full = clip_scale * (embed_grad + head_grad)
    new_v = beta_two * moment_v + (1.0 - beta_two) * (grad_full * grad_full + 1e-30)
    new_m = 0.9 * moment_m + 0.1 * (grad_full / jnp.sqrt(new_v))
    new_w = master_w - learn_rate * new_m - learn_rate * learn_rate * master_w
    return new_w, new_m, new_v


def iota(shape, dim):
    return lax.broadcasted_iota(I32, shape, dim)


def onehot(cond):
    return jnp.where(cond, 1.0, 0.0).astype(BF16)


def slots_hot(slots, first, cap):
    row = (slots - first).astype(I16)
    return jnp.where(lax.broadcasted_iota(I16, (cap, slots.shape[1]), 0) == row, BF16(1), BF16(0))


def dot_nt(a, b):
    return lax.dot_general(a, b, (((1,), (1,)), ((), ())), preferred_element_type=F32)


def dot_nn(a, b):
    return jnp.dot(a, b, preferred_element_type=F32)


def ranks(pres, group):
    rows = pres.shape[0]
    pres_b = pres.astype(BF16)
    before = onehot(iota((KW, KW), 0) < iota((KW, KW), 1))
    inner = dot_nn(pres_b, before)
    if group > 1:
        r, c = iota((rows, rows), 0), iota((rows, rows), 1)
        above = onehot((c < r) & (c // group == r // group))
        inner = inner + jnp.sum(dot_nn(above, pres_b), axis=1, keepdims=True)
    return inner.astype(I32)


def codes(pres, group, cap):
    rows = pres.shape[0]
    rank = ranks(pres, group)
    code = jnp.where((pres > 0.5) & (rank < cap), (iota((rows, KW), 0) // group) * cap + rank + 1, 0)
    over = jnp.where((pres > 0.5) & (rank >= cap), 1.0, 0.0)
    return code, jnp.max(over)


def index_first(coords, tok_ref, slot_ref, tables):
    ids = jnp.concatenate([tok_ref[r:r + 1] for r in range(tok_ref.shape[0])], axis=1)
    tp, c1, c2, c3 = coords
    x, y, z = ids & 3, (ids >> 2) & 3, (ids >> 4) & 3
    d1 = x + (z - x) * tp
    d2 = y + (x - y) * tp
    d3 = z + (y - z) * tp
    q = (((d1 - c1) & 3) << 4) + (((d2 - c2) & 3) << 2) + ((d3 - c3) & 3)
    upper = ids >= 16064
    kk = jnp.where(upper, ids - 16064, ids) >> 6
    k = jnp.where(upper, 256, 0) + ((kk & 1) << 7) + (kk >> 1)
    n = ids.shape[1]
    hot_q = onehot(iota((64, n), 0) == q)
    hot_k = onehot(iota((KW, n), 0) == k)
    pres = jnp.minimum(dot_nt(hot_q, hot_k), 1.0)
    code, over = codes(pres, 16, CAP[0])
    both = jnp.concatenate([(code >> 5).astype(BF16), (code & 31).astype(BF16)], axis=0)
    found = dot_nn(both, hot_k)
    value = found[:64] * 32.0 + found[64:]
    slot_ref[...] = jnp.sum(jnp.where(iota((64, n), 0) == q, value, 0.0), axis=0, keepdims=True).astype(I32) - 1
    for o in range(4):
        tables[o] = pres[16 * o:16 * o + 16]
    return over


def gather_first(o, slot_ref, rows_ref, outs, start):
    cap, depth = outs[0].shape[0], 1024
    columns = pl.ds(start, CHUNK * len(outs))

    def step(n, first):
        at = pl.ds(pl.multiple_of(n * depth, depth), depth)
        part = dot_nn(slots_hot(slot_ref[:, at], o * cap, cap), rows_ref[at, columns])
        for chunk, out in enumerate(outs):
            piece = part[:, CHUNK * chunk:CHUNK * chunk + CHUNK]
            out[...] = piece if first else out[...] + piece

    step(0, True)
    lax.fori_loop(1, rows_ref.shape[0] // depth, lambda n, c: (step(n, False), c)[1], 0)


def index_next(group, cap_in, cap_out, blocks, slot_ref, tables):
    rows = 4 * group
    blocks = [block[:rows] for block in blocks]
    merged = jnp.minimum(blocks[0] + blocks[1] + blocks[2] + blocks[3], 1.0)
    code, over = codes(merged, group, cap_out)
    hi, lo = (code >> 5).astype(F32), (code & 31).astype(F32)
    every = jnp.concatenate(blocks, axis=0)
    every = jnp.where(every > 0.5, ranks(every, rows), -1)
    spread = onehot((iota((16, KW), 1) >> 5) == iota((16, KW), 0))
    own_row = (iota((32, KW), 1) & 31) == iota((32, KW), 0)
    found = []
    for s in range(4):
        highs, lows = [], []
        for r in range(rows):
            row = every[rows * s + r:rows * s + r + 1]
            highs.append(onehot(iota((16, KW), 0) == (row >> 5)))
            low = iota((32, KW), 0) == (row & 31)
            low = jnp.concatenate([jnp.where(low, hi[r:r + 1], 0.0), jnp.where(low, lo[r:r + 1], 0.0)], axis=0)
            lows.append(low.astype(BF16))
        table = dot_nt(jnp.concatenate(lows, axis=1), jnp.concatenate(highs, axis=1)).astype(BF16)
        value = dot_nn(table, spread)
        value = jnp.where(own_row, value[:32] * 32.0 + value[32:], 0.0)
        found.append(jnp.sum(value, axis=0, keepdims=True)[:, :cap_in])
    slot_ref[:, :4 * cap_in] = jnp.concatenate(found, axis=1).astype(I32) - 1
    tables[...] = jnp.zeros(tables.shape, F32)
    for o in range(4):
        tables[o, :group] = merged[group * o:group * o + group]
    return over


def split_rows(rows):
    high = jnp.clip(rows, -3.38e38, 3.38e38).astype(BF16)
    rest = rows - high.astype(F32)
    mid = rest.astype(BF16)
    return high, mid, (rest - mid.astype(F32)).astype(BF16)


def split_blocks(blocks, pieces):
    cap = blocks[0].shape[0]
    for s, rows in enumerate(blocks):
        for n, piece in enumerate(split_rows(rows[...])):
            pieces[n, cap * s:cap * s + cap] = piece


def gather_next(o, depth, slot_ref, pieces, out_ref):
    cap = out_ref.shape[0]
    hot = slots_hot(slot_ref[:, :depth], o * cap, cap)
    out_ref[...] = dot_nn(hot, pieces[0, :depth]) + dot_nn(hot, pieces[1, :depth]) + dot_nn(hot, pieces[2, :depth])


def dense_last(tables, blocks, flag, out_ref):
    pres = jnp.concatenate([table[...] for table in tables], axis=0)
    rank = jnp.where(pres > 0.5, ranks(pres, 1), -1)
    cap = blocks[0].shape[0]
    hot = jnp.concatenate([slots_hot(rank[8 * s:8 * s + 1], 0, cap) for s in range(4)], axis=0)
    rows = jnp.concatenate([block[...] for block in blocks], axis=0).T
    high, mid, low = split_rows(rows)
    total = dot_nn(high, hot) + dot_nn(mid, hot) + dot_nn(low, hot)
    total = jnp.where((iota(total.shape, 1) & 255) == 255, flag, total)
    for t in range(2):
        out_ref[t] = total[:, 256 * t:256 * t + 256].reshape(out_ref.shape[1:])


def assemble(tok_ref, rows_ref, head_ref, w_ref, m_ref, v_ref, recv_ref, head_out, w_out, m_out, v_out, half, slot1, slot2, slot3, tab1, tab2, tab3, rtab1, rtab2, rtab3, send1, send2, send3,
             recv1, recv2, recv3, pieces, own_over, peer_over, dense, table_sem, half_sem, tab_out, tab_in, row_out, row_in, over_out, over_in, last_out, last_in):
    tp, me = lax.axis_index("tp"), lax.axis_index("fsdp")
    ring = []
    for low, high in STRIDES:
        stride = low + (high - low) * tp
        ring.append((stride, (me // stride) % 4))
    coords = (tp, *(at for _, at in ring))
    width = half.shape[1]
    same = 1 - (me // 32 + tp) % 2

    def neighbour(phase, offset):
        stride, at = ring[phase]
        return {"fsdp": me + stride * ((at + offset) % 4 - at)}

    barrier = pltpu.get_barrier_semaphore()

    def greet(device):
        pl.semaphore_signal(barrier, inc=1, device_id=device, device_id_type=MESH)

    for phase in range(3):
        for o in (1, 2, 3):
            greet(neighbour(phase, o))
    greet({"tp": 1 - tp})

    load = pltpu.make_async_copy(rows_ref.at[:, pl.ds(pl.multiple_of(tp * width, width), width)], half, half_sem)
    load.start()
    over = index_first(coords, tok_ref, slot1, tab1)
    pl.semaphore_wait(barrier, 10)
    loads = [pltpu.make_async_copy(src, dst, table_sem.at[n])
             for n, (src, dst) in enumerate(((head_ref, head_out), (w_ref, w_out), (m_ref, m_out), (v_ref, v_out)))]

    def copy_to(src, dst, out, into, device):
        return pltpu.make_async_remote_copy(
            src_ref=src, dst_ref=dst, send_sem=out, recv_sem=into, device_id=device, device_id_type=MESH)

    def remote(*args):
        copy = copy_to(*args)
        copy.start()
        return copy

    def send_tables(phase, table, into):
        return [remote(table.at[o], into.at[o - 1], tab_out.at[3 * phase + o - 1], tab_in.at[3 * phase + o - 1], neighbour(phase, o))
                for o in (1, 2, 3)]

    def send_row(phase, chunk, o, rows, into):
        sem = 6 * phase + 3 * chunk + o - 1
        return copy_to(rows.at[chunk, o], into.at[chunk, o - 1], row_out.at[sem], row_in.at[sem], neighbour(phase, o))

    def wait(copies):
        for copy in copies:
            copy.wait()

    def beside(own, got):
        return [own.at[0], *(got.at[n] for n in range(3))]

    def loop_bins(step):
        lax.fori_loop(0, 3, lambda n, c: (step(2 - n + 3 * (n // 2)), c)[1], 0)

    def first(*chunks):
        def step(o):
            gather_first(o, slot1, half, [send1.at[chunk, o] for chunk in chunks], CHUNK * chunks[0])

        return step

    def first_sent(chunk):
        def step(o):
            first(chunk)(o)
            send_row(0, chunk, o, send1, recv1).start()

        return step

    def later(phase, chunk, hold=False):
        slot, own, got, out, into = ((slot2, send1, recv1, send2, recv2), (slot3, send2, recv2, send3, recv3))[phase - 1]
        blocks = beside(own.at[chunk], got.at[chunk])
        depth = 4 * CAP[phase - 1]
        split_blocks(blocks, pieces)

        def sent(o):
            gather_next(o, depth, slot, pieces, out.at[chunk, o])
            if hold:
                pl.when(tp == 0)(send_row(phase, chunk, o, out, into).start)
            else:
                send_row(phase, chunk, o, out, into).start()

        loop_bins(sent)
        if hold:
            @pl.when(tp == 1)
            def _():
                wait_rows(0, 1)
                for o in (2, 1, 3):
                    send_row(phase, chunk, o, out, into).start()

        gather_next(0, depth, slot, pieces, out.at[chunk, 0])

    def wait_rows(phase, chunk):
        out, into = ((send1, recv1), (send2, recv2), (send3, recv3))[phase]
        for o in (1, 2, 3):
            send_row(phase, chunk, o, out, into).wait()

    def finish_chunk(chunk):
        dense_last(beside(tab3, rtab3), beside(send3.at[chunk], recv3.at[chunk]), flag, dense.at[chunk])

    tables1 = send_tables(0, tab1, rtab1)
    load.wait()
    loop_bins(first_sent(0))
    loop_bins(first_sent(1))
    for table in loads:
        table.start()
    wait(tables1)
    over = jnp.maximum(over, index_next(4, CAP[0], CAP[1], beside(tab1, rtab1), slot2, tab2))
    tables2 = send_tables(1, tab2, rtab2)
    first(0, 1)(0)
    wait(tables2)
    over = jnp.maximum(over, index_next(1, CAP[1], CAP[2], beside(tab2, rtab2), slot3, tab3))
    own_over[...] = jnp.full(own_over.shape, over, F32)
    tables3 = send_tables(2, tab3, rtab3)
    tables3.append(remote(own_over, peer_over, over_out, over_in, {"tp": 1 - tp}))
    wait_rows(0, 0)

    later(1, 0, hold=True)

    @pl.when(tp == 0)
    def _():
        wait_rows(0, 1)

    later(1, 1)
    wait_rows(1, 0)
    later(2, 0)
    wait(tables3)
    flag = jnp.maximum(own_over[0:1, 0:1], peer_over[0:1, 0:1])
    wait_rows(1, 1)
    later(2, 1)
    wait_rows(2, 0)
    finish_chunk(0)

    def last(i, far):
        at = (me + i) % 32
        core = (tp + far) % 2
        return pltpu.make_async_remote_copy(
            src_ref=dense.at[at // 16, core, at % 16], dst_ref=recv_ref.at[me], send_sem=last_out.at[2 * i + far],
            recv_sem=last_in.at[me], device_id={"fsdp": 32 * tp + at, "tp": core}, device_id_type=MESH)

    def arrive(j):
        return pltpu.make_async_remote_copy(
            src_ref=dense.at[0, 0, 0], dst_ref=recv_ref.at[j], send_sem=last_out.at[0], recv_sem=last_in.at[j],
            device_id={"tp": 1 - tp}, device_id_type=MESH)

    def each_pair(chunk, act, self_act):
        def pair(n, carry):
            at = 16 * chunk + (7 * me + 5 * (me // 16) + n) % 16
            i = (at - me % 32 + 32) % 32
            act(last(i, 1))

            @pl.when((same == 0) | (i > 0))
            def _():
                act(last(i, 0))

            @pl.when((same == 1) & (i == 0))
            def _():
                self_act()

            return carry

        lax.fori_loop(0, 16, pair, 0)

    def keep():
        recv_ref[me] = dense[(me % 32) // 16, tp, me % 16]

    each_pair(0, lambda copy: copy.start(), keep)
    wait_rows(2, 1)
    finish_chunk(1)
    each_pair(1, lambda copy: copy.start(), keep)

    def wait_arrival(i, carry):
        arrive((me + i) % 64).wait_recv()
        return carry

    lax.fori_loop(1, 64, wait_arrival, 0)

    @pl.when(same == 0)
    def _():
        arrive(me).wait_recv()

    wait(loads)
    each_pair(0, lambda copy: copy.wait_send(), lambda: None)
    each_pair(1, lambda copy: copy.wait_send(), lambda: None)


def finish(lr_ref, clip_ref, recv_ref, head_ref, w_ref, m_ref, v_ref, w_out, m_out, v_out, b_out, grad):
    tiles = grad.shape[0]
    for c in range(16):
        both = jnp.concatenate([recv_ref[:, c, :128], recv_ref[:, c, 128:]], axis=0)
        grad[:, c, :] = both.T[:tiles]
    lr, clip = lr_ref[0, 0], clip_ref[0, 0]
    rows = head_ref.shape[1]
    for t in range(tiles):
        at = slice(128 * t, min(128 * t + 128, rows))
        width = at.stop - at.start
        new_w, new_m, new_v = update_math(grad[t, :, :width], head_ref[:, at], w_ref[:, at], m_ref[:, at], v_ref[:, at], lr, clip)
        w_out[:, at], m_out[:, at], v_out[:, at] = new_w, new_m, new_v
        b_out[:, at] = new_w.astype(BF16)


def shaped(*shape, dtype=F32):
    return jax.ShapeDtypeStruct(shape, dtype)


def dense_rows(ids_ref, rows_ref, out_ref):
    first = pl.program_id(0) * out_ref.shape[0]
    hot = onehot(iota((out_ref.shape[0], rows_ref.shape[0]), 0) + first == ids_ref[...])
    part = dot_nn(hot, rows_ref[...])

    @pl.when(pl.program_id(1) == 0)
    def _():
        out_ref[...] = part

    @pl.when(pl.program_id(1) > 0)
    def _():
        out_ref[...] += part


def solution(mesh):
    row_spec = P(("dp", "fsdp"), None)
    act_spec = P(("dp", "fsdp"), None, None)
    table_spec = P(("dp", "tp"), "fsdp")

    def dense_grad(ids, rows, shard_rows):
        n, width = rows.shape
        block, depth = 256, 1024
        tiles = -(-shard_rows // block)
        part = pl.pallas_call(
            dense_rows,
            grid=(tiles, n // depth),
            in_specs=[pl.BlockSpec((1, depth), lambda i, k: (0, k)), pl.BlockSpec((depth, width), lambda i, k: (k, 0))],
            out_specs=pl.BlockSpec((block, width), lambda i, k: (i, 0)),
            out_shape=shaped(tiles * block, width),
            compiler_params=pltpu.CompilerParams(vmem_limit_bytes=VLIM),
            name="dense_rows",
        )(ids - lax.axis_index("tp") * shard_rows, rows)
        part = part[:shard_rows].T.reshape(64, 16, shard_rows)
        return jnp.sum(lax.all_to_all(part, "fsdp", 0, 0, tiled=True), axis=0)

    def local_step(tokens, out_grad, head_grad, master_w, moment_m, moment_v, learn_rate, clip_scale):
        n = tokens.size
        rows = out_grad.reshape(n, -1)
        width = rows.shape[1] // 2
        vm, dma = pltpu.VMEM, pltpu.SemaphoreType.DMA
        tables = (head_grad.T, master_w.T, moment_m.T, moment_v.T)
        shard_rows = master_w.shape[0]
        shard = (16, shard_rows)
        recv, *near = pl.pallas_call(
            assemble,
            out_shape=(shaped(64, 16, 256), *[shaped(*shard)] * 4),
            in_specs=[pl.BlockSpec(memory_space=vm)] + [pl.BlockSpec(memory_space=pl.ANY)] * 5,
            out_specs=tuple([pl.BlockSpec(memory_space=vm)] * 5),
            scratch_shapes=[
                vm((n, width), BF16), vm((1, n), I32), vm((1, 4 * KW), I32), vm((1, 4 * KW), I32),
                vm((4, 16, KW), F32), vm((4, 8, KW), F32), vm((4, 8, KW), F32),
                vm((3, 16, KW), F32), vm((3, 8, KW), F32), vm((3, 8, KW), F32),
                *[vm((2, 4, cap, CHUNK), F32) for cap in CAP],
                *[vm((2, 3, cap, CHUNK), F32) for cap in CAP],
                vm((3, 4 * CAP[0], CHUNK), BF16),
                vm((8, 128), F32), vm((8, 128), F32), vm((2, 2, 16, 16, 256), F32),
                dma((4,)), dma, dma((9,)), dma((9,)), dma((18,)), dma((18,)), dma, dma, dma((64,)), dma((64,)),
            ],
            compiler_params=pltpu.CompilerParams(vmem_limit_bytes=40 << 20, collective_id=0, has_side_effects=True),
            name="assemble",
        )(tokens, rows, *tables)
        flag = jnp.max(recv[:, 0, 255]) > 0.5

        def fast(_):
            vm, scalar = pl.BlockSpec(memory_space=pltpu.VMEM), pl.BlockSpec(memory_space=pltpu.SMEM)
            return pl.pallas_call(
                finish,
                out_shape=(shaped(*shard), shaped(*shard), shaped(*shard), shaped(*shard, dtype=BF16)),
                in_specs=[scalar, scalar, vm, vm, vm, vm, vm],
                out_specs=(vm, vm, vm, vm),
                scratch_shapes=[pltpu.VMEM(((shard_rows + 127) // 128, 16, 128), F32)],
                compiler_params=pltpu.CompilerParams(vmem_limit_bytes=VLIM),
                name="finish",
            )(learn_rate.reshape(1, 1), clip_scale.reshape(1, 1), recv, *near)

        def slow(_):
            grad = dense_grad(tokens.reshape(1, -1), rows, shard_rows)
            new_w, new_m, new_v = update_math(grad, *tables, learn_rate, clip_scale)
            return new_w, new_m, new_v, new_w.astype(BF16)

        return tuple(a.T for a in lax.cond(flag, slow, fast, None))

    return jax.shard_map(local_step, mesh=mesh, in_specs=(row_spec, act_spec, table_spec, table_spec, table_spec, table_spec, P(), P()), out_specs=(table_spec, table_spec, table_spec, table_spec), check_vma=False)
```

```python
import functools

import jax
import jax.numpy as jnp
from jax import lax
from jax.experimental import pallas as pl
from jax.experimental.pallas import tpu as pltpu
from jax.sharding import PartitionSpec as P

OPT_STEP = 20
F32, BF16, I32, I16 = jnp.float32, jnp.bfloat16, jnp.int32, jnp.int16
CAP = (480, 352, 208)
KW = 512
STRIDES = ((1, 16), (4, 1), (16, 4))
VLIM = 20 << 20
MESH = pl.DeviceIdType.MESH
CHUNK = 256


def update_math(embed_grad, head_grad, master_w, moment_m, moment_v, learn_rate, clip_scale):
    beta_two = 1.0 - OPT_STEP ** -0.8
    grad_full = clip_scale * (embed_grad + head_grad)
    new_v = beta_two * moment_v + (1.0 - beta_two) * (grad_full * grad_full + 1e-30)
    new_m = 0.9 * moment_m + 0.1 * (grad_full / jnp.sqrt(new_v))
    new_w = master_w - learn_rate * new_m - learn_rate * learn_rate * master_w
    return new_w, new_m, new_v


def iota(shape, dim):
    return lax.broadcasted_iota(I32, shape, dim)


def onehot(cond):
    return jnp.where(cond, 1.0, 0.0).astype(BF16)


def slots_hot(slots, first, cap):
    row = (slots - first).astype(I16)
    return jnp.where(lax.broadcasted_iota(I16, (cap, slots.shape[1]), 0) == row, BF16(1), BF16(0))


def dot_nt(a, b):
    return lax.dot_general(a, b, (((1,), (1,)), ((), ())), preferred_element_type=F32)


def dot_nn(a, b):
    return jnp.dot(a, b, preferred_element_type=F32)


def ranks(pres, group):
    rows = pres.shape[0]
    pres_b = pres.astype(BF16)
    before = onehot(iota((KW, KW), 0) < iota((KW, KW), 1))
    inner = dot_nn(pres_b, before)
    if group > 1:
        r, c = iota((rows, rows), 0), iota((rows, rows), 1)
        above = onehot((c < r) & (c // group == r // group))
        inner = inner + jnp.sum(dot_nn(above, pres_b), axis=1, keepdims=True)
    return inner.astype(I32)


def codes(pres, group, cap):
    rows = pres.shape[0]
    rank = ranks(pres, group)
    code = jnp.where((pres > 0.5) & (rank < cap), (iota((rows, KW), 0) // group) * cap + rank + 1, 0)
    over = jnp.where((pres > 0.5) & (rank >= cap), 1.0, 0.0)
    return code, jnp.max(over)


def index_first(coords, tok_ref, slot_ref, tables):
    ids = jnp.concatenate([tok_ref[r:r + 1] for r in range(tok_ref.shape[0])], axis=1)
    tp, c1, c2, c3 = coords
    x, y, z = ids & 3, (ids >> 2) & 3, (ids >> 4) & 3
    d1 = x + (z - x) * tp
    d2 = y + (x - y) * tp
    d3 = z + (y - z) * tp
    q = (((d1 - c1) & 3) << 4) + (((d2 - c2) & 3) << 2) + ((d3 - c3) & 3)
    upper = ids >= 16064
    kk = jnp.where(upper, ids - 16064, ids) >> 6
    k = jnp.where(upper, 256, 0) + ((kk & 1) << 7) + (kk >> 1)
    n = ids.shape[1]
    hot_q = onehot(iota((64, n), 0) == q)
    hot_k = onehot(iota((KW, n), 0) == k)
    pres = jnp.minimum(dot_nt(hot_q, hot_k), 1.0)
    code, over = codes(pres, 16, CAP[0])
    both = jnp.concatenate([(code >> 5).astype(BF16), (code & 31).astype(BF16)], axis=0)
    found = dot_nn(both, hot_k)
    value = found[:64] * 32.0 + found[64:]
    slot_ref[...] = jnp.sum(jnp.where(iota((64, n), 0) == q, value, 0.0), axis=0, keepdims=True).astype(I32) - 1
    for o in range(4):
        tables[o] = pres[16 * o:16 * o + 16]
    return over


def gather_first(o, slot_ref, rows_ref, outs, start):
    cap, depth = outs[0].shape[0], 1024
    columns = pl.ds(start, CHUNK * len(outs))

    def step(n, first):
        at = pl.ds(pl.multiple_of(n * depth, depth), depth)
        part = dot_nn(slots_hot(slot_ref[:, at], o * cap, cap), rows_ref[at, columns])
        for chunk, out in enumerate(outs):
            piece = part[:, CHUNK * chunk:CHUNK * chunk + CHUNK]
            out[...] = piece if first else out[...] + piece

    step(0, True)
    lax.fori_loop(1, rows_ref.shape[0] // depth, lambda n, c: (step(n, False), c)[1], 0)


def index_next(group, cap_in, cap_out, blocks, slot_ref, tables):
    rows = 4 * group
    blocks = [block[:rows] for block in blocks]
    merged = jnp.minimum(blocks[0] + blocks[1] + blocks[2] + blocks[3], 1.0)
    code, over = codes(merged, group, cap_out)
    hi, lo = (code >> 5).astype(F32), (code & 31).astype(F32)
    every = jnp.concatenate(blocks, axis=0)
    every = jnp.where(every > 0.5, ranks(every, rows), -1)
    spread = onehot((iota((16, KW), 1) >> 5) == iota((16, KW), 0))
    own_row = (iota((32, KW), 1) & 31) == iota((32, KW), 0)
    found = []
    for s in range(4):
        highs, lows = [], []
        for r in range(rows):
            row = every[rows * s + r:rows * s + r + 1]
            highs.append(onehot(iota((16, KW), 0) == (row >> 5)))
            low = iota((32, KW), 0) == (row & 31)
            low = jnp.concatenate([jnp.where(low, hi[r:r + 1], 0.0), jnp.where(low, lo[r:r + 1], 0.0)], axis=0)
            lows.append(low.astype(BF16))
        table = dot_nt(jnp.concatenate(lows, axis=1), jnp.concatenate(highs, axis=1)).astype(BF16)
        value = dot_nn(table, spread)
        value = jnp.where(own_row, value[:32] * 32.0 + value[32:], 0.0)
        found.append(jnp.sum(value, axis=0, keepdims=True)[:, :cap_in])
    slot_ref[:, :4 * cap_in] = jnp.concatenate(found, axis=1).astype(I32) - 1
    tables[...] = jnp.zeros(tables.shape, F32)
    for o in range(4):
        tables[o, :group] = merged[group * o:group * o + group]
    return over


def split_rows(rows):
    high = jnp.clip(rows, -3.38e38, 3.38e38).astype(BF16)
    rest = rows - high.astype(F32)
    mid = rest.astype(BF16)
    return high, mid, (rest - mid.astype(F32)).astype(BF16)


def split_blocks(blocks, pieces):
    cap = blocks[0].shape[0]
    for s, rows in enumerate(blocks):
        for n, piece in enumerate(split_rows(rows[...])):
            pieces[n, cap * s:cap * s + cap] = piece


def gather_next(o, depth, slot_ref, pieces, out_ref):
    cap = out_ref.shape[0]
    hot = slots_hot(slot_ref[:, :depth], o * cap, cap)
    out_ref[...] = dot_nn(hot, pieces[0, :depth]) + dot_nn(hot, pieces[1, :depth]) + dot_nn(hot, pieces[2, :depth])


def dense_last(tables, blocks, flag, out_ref):
    pres = jnp.concatenate([table[...] for table in tables], axis=0)
    rank = jnp.where(pres > 0.5, ranks(pres, 1), -1)
    cap = blocks[0].shape[0]
    hot = jnp.concatenate([slots_hot(rank[8 * s:8 * s + 1], 0, cap) for s in range(4)], axis=0)
    rows = jnp.concatenate([block[...] for block in blocks], axis=0).T
    high, mid, low = split_rows(rows)
    total = dot_nn(high, hot) + dot_nn(mid, hot) + dot_nn(low, hot)
    total = jnp.where((iota(total.shape, 1) & 255) == 255, flag, total)
    for t in range(2):
        out_ref[t] = total[:, 256 * t:256 * t + 256].reshape(out_ref.shape[1:])


def assemble(tok_ref, rows_ref, head_ref, w_ref, m_ref, v_ref, recv_ref, head_out, w_out, m_out, v_out, half, slot1, slot2, slot3, tab1, tab2, tab3, rtab1, rtab2, rtab3, send1, send2, send3,
             recv1, recv2, recv3, pieces, own_over, peer_over, dense, table_sem, half_sem, tab_out, tab_in, row_out, row_in, over_out, over_in, last_out, last_in):
    tp, me = lax.axis_index("tp"), lax.axis_index("fsdp")
    ring = []
    for low, high in STRIDES:
        stride = low + (high - low) * tp
        ring.append((stride, (me // stride) % 4))
    coords = (tp, *(at for _, at in ring))
    width = half.shape[1]
    same = 1 - (me // 32 + tp) % 2

    def neighbour(phase, offset):
        stride, at = ring[phase]
        return {"fsdp": me + stride * ((at + offset) % 4 - at)}

    barrier = pltpu.get_barrier_semaphore()

    def greet(device):
        pl.semaphore_signal(barrier, inc=1, device_id=device, device_id_type=MESH)

    for phase in range(3):
        for o in (1, 2, 3):
            greet(neighbour(phase, o))
    greet({"tp": 1 - tp})

    load = pltpu.make_async_copy(rows_ref.at[:, pl.ds(pl.multiple_of(tp * width, width), width)], half, half_sem)
    load.start()
    over = index_first(coords, tok_ref, slot1, tab1)
    pl.semaphore_wait(barrier, 10)
    loads = [pltpu.make_async_copy(src, dst, table_sem.at[n])
             for n, (src, dst) in enumerate(((head_ref, head_out), (w_ref, w_out), (m_ref, m_out), (v_ref, v_out)))]

    def copy_to(src, dst, out, into, device):
        return pltpu.make_async_remote_copy(
            src_ref=src, dst_ref=dst, send_sem=out, recv_sem=into, device_id=device, device_id_type=MESH)

    def remote(*args):
        copy = copy_to(*args)
        copy.start()
        return copy

    def send_tables(phase, table, into):
        return [remote(table.at[o], into.at[o - 1], tab_out.at[3 * phase + o - 1], tab_in.at[3 * phase + o - 1], neighbour(phase, o))
                for o in (1, 2, 3)]

    def send_row(phase, chunk, o, rows, into):
        sem = 6 * phase + 3 * chunk + o - 1
        return copy_to(rows.at[chunk, o], into.at[chunk, o - 1], row_out.at[sem], row_in.at[sem], neighbour(phase, o))

    def wait(copies):
        for copy in copies:
            copy.wait()

    def beside(own, got):
        return [own.at[0], *(got.at[n] for n in range(3))]

    def loop_bins(step):
        lax.fori_loop(0, 3, lambda n, c: (step(2 - n + 3 * (n // 2)), c)[1], 0)

    def first(*chunks):
        def step(o):
            gather_first(o, slot1, half, [send1.at[chunk, o] for chunk in chunks], CHUNK * chunks[0])

        return step

    def first_sent(chunk):
        def step(o):
            first(chunk)(o)
            send_row(0, chunk, o, send1, recv1).start()

        return step

    def later(phase, chunk, hold=False):
        slot, own, got, out, into = ((slot2, send1, recv1, send2, recv2), (slot3, send2, recv2, send3, recv3))[phase - 1]
        blocks = beside(own.at[chunk], got.at[chunk])
        depth = 4 * CAP[phase - 1]
        split_blocks(blocks, pieces)

        def sent(o):
            gather_next(o, depth, slot, pieces, out.at[chunk, o])
            if hold:
                pl.when(tp == 0)(send_row(phase, chunk, o, out, into).start)
            else:
                send_row(phase, chunk, o, out, into).start()

        loop_bins(sent)
        if hold:
            @pl.when(tp == 1)
            def _():
                wait_rows(0, 1)
                for o in (2, 1, 3):
                    send_row(phase, chunk, o, out, into).start()

        gather_next(0, depth, slot, pieces, out.at[chunk, 0])

    def wait_rows(phase, chunk):
        out, into = ((send1, recv1), (send2, recv2), (send3, recv3))[phase]
        for o in (1, 2, 3):
            send_row(phase, chunk, o, out, into).wait()

    def finish_chunk(chunk):
        dense_last(beside(tab3, rtab3), beside(send3.at[chunk], recv3.at[chunk]), flag, dense.at[chunk])

    tables1 = send_tables(0, tab1, rtab1)
    load.wait()
    loop_bins(first_sent(0))
    loop_bins(first_sent(1))
    for table in loads:
        table.start()
    wait(tables1)
    over = jnp.maximum(over, index_next(4, CAP[0], CAP[1], beside(tab1, rtab1), slot2, tab2))
    tables2 = send_tables(1, tab2, rtab2)
    first(0, 1)(0)
    wait(tables2)
    over = jnp.maximum(over, index_next(1, CAP[1], CAP[2], beside(tab2, rtab2), slot3, tab3))
    own_over[...] = jnp.full(own_over.shape, over, F32)
    tables3 = send_tables(2, tab3, rtab3)
    tables3.append(remote(own_over, peer_over, over_out, over_in, {"tp": 1 - tp}))
    wait_rows(0, 0)

    later(1, 0, hold=True)

    @pl.when(tp == 0)
    def _():
        wait_rows(0, 1)

    later(1, 1)
    wait_rows(1, 0)
    later(2, 0)
    wait(tables3)
    flag = jnp.maximum(own_over[0:1, 0:1], peer_over[0:1, 0:1])
    def last(i, far):
        at = (me + i) % 32
        core = (tp + far) % 2
        return pltpu.make_async_remote_copy(
            src_ref=dense.at[at // 16, core, at % 16], dst_ref=recv_ref.at[me], send_sem=last_out.at[2 * i + far],
            recv_sem=last_in.at[me], device_id={"fsdp": 32 * tp + at, "tp": core}, device_id_type=MESH)

    def arrive(j):
        return pltpu.make_async_remote_copy(
            src_ref=dense.at[0, 0, 0], dst_ref=recv_ref.at[j], send_sem=last_out.at[0], recv_sem=last_in.at[j],
            device_id={"tp": 1 - tp}, device_id_type=MESH)

    def each_pair(chunk, act, self_act):
        def pair(n, carry):
            at = 16 * chunk + (7 * me + 5 * (me // 16) + n) % 16
            i = (at - me % 32 + 32) % 32
            act(last(i, 1))

            @pl.when((same == 0) | (i > 0))
            def _():
                act(last(i, 0))

            @pl.when((same == 1) & (i == 0))
            def _():
                self_act()

            return carry

        lax.fori_loop(0, 16, pair, 0)

    def keep():
        recv_ref[me] = dense[(me % 32) // 16, tp, me % 16]

    @pl.when(tp == 0)
    def _():
        wait_rows(2, 0)
        finish_chunk(0)
        each_pair(0, lambda copy: copy.start(), keep)

    wait_rows(1, 1)
    later(2, 1)

    @pl.when(tp == 1)
    def _():
        wait_rows(2, 0)
        finish_chunk(0)
        each_pair(0, lambda copy: copy.start(), keep)

    wait_rows(2, 1)
    finish_chunk(1)
    each_pair(1, lambda copy: copy.start(), keep)

    def wait_arrival(i, carry):
        arrive((me + i) % 64).wait_recv()
        return carry

    lax.fori_loop(1, 64, wait_arrival, 0)

    @pl.when(same == 0)
    def _():
        arrive(me).wait_recv()

    wait(loads)
    each_pair(0, lambda copy: copy.wait_send(), lambda: None)
    each_pair(1, lambda copy: copy.wait_send(), lambda: None)


def finish(lr_ref, clip_ref, recv_ref, head_ref, w_ref, m_ref, v_ref, w_out, m_out, v_out, b_out, grad):
    tiles = grad.shape[0]
    for c in range(16):
        both = jnp.concatenate([recv_ref[:, c, :128], recv_ref[:, c, 128:]], axis=0)
        grad[:, c, :] = both.T[:tiles]
    lr, clip = lr_ref[0, 0], clip_ref[0, 0]
    rows = head_ref.shape[1]
    for t in range(tiles):
        at = slice(128 * t, min(128 * t + 128, rows))
        width = at.stop - at.start
        new_w, new_m, new_v = update_math(grad[t, :, :width], head_ref[:, at], w_ref[:, at], m_ref[:, at], v_ref[:, at], lr, clip)
        w_out[:, at], m_out[:, at], v_out[:, at] = new_w, new_m, new_v
        b_out[:, at] = new_w.astype(BF16)


def shaped(*shape, dtype=F32):
    return jax.ShapeDtypeStruct(shape, dtype)


def dense_rows(ids_ref, rows_ref, out_ref):
    first = pl.program_id(0) * out_ref.shape[0]
    hot = onehot(iota((out_ref.shape[0], rows_ref.shape[0]), 0) + first == ids_ref[...])
    part = dot_nn(hot, rows_ref[...])

    @pl.when(pl.program_id(1) == 0)
    def _():
        out_ref[...] = part

    @pl.when(pl.program_id(1) > 0)
    def _():
        out_ref[...] += part


def solution(mesh):
    row_spec = P(("dp", "fsdp"), None)
    act_spec = P(("dp", "fsdp"), None, None)
    table_spec = P(("dp", "tp"), "fsdp")

    def dense_grad(ids, rows, shard_rows):
        n, width = rows.shape
        block, depth = 256, 1024
        tiles = -(-shard_rows // block)
        part = pl.pallas_call(
            dense_rows,
            grid=(tiles, n // depth),
            in_specs=[pl.BlockSpec((1, depth), lambda i, k: (0, k)), pl.BlockSpec((depth, width), lambda i, k: (k, 0))],
            out_specs=pl.BlockSpec((block, width), lambda i, k: (i, 0)),
            out_shape=shaped(tiles * block, width),
            compiler_params=pltpu.CompilerParams(vmem_limit_bytes=VLIM),
            name="dense_rows",
        )(ids - lax.axis_index("tp") * shard_rows, rows)
        part = part[:shard_rows].T.reshape(64, 16, shard_rows)
        return jnp.sum(lax.all_to_all(part, "fsdp", 0, 0, tiled=True), axis=0)

    def local_step(tokens, out_grad, head_grad, master_w, moment_m, moment_v, learn_rate, clip_scale):
        n = tokens.size
        rows = out_grad.reshape(n, -1)
        width = rows.shape[1] // 2
        vm, dma = pltpu.VMEM, pltpu.SemaphoreType.DMA
        tables = (head_grad.T, master_w.T, moment_m.T, moment_v.T)
        shard_rows = master_w.shape[0]
        shard = (16, shard_rows)
        recv, *near = pl.pallas_call(
            assemble,
            out_shape=(shaped(64, 16, 256), *[shaped(*shard)] * 4),
            in_specs=[pl.BlockSpec(memory_space=vm)] + [pl.BlockSpec(memory_space=pl.ANY)] * 5,
            out_specs=tuple([pl.BlockSpec(memory_space=vm)] * 5),
            scratch_shapes=[
                vm((n, width), BF16), vm((1, n), I32), vm((1, 4 * KW), I32), vm((1, 4 * KW), I32),
                vm((4, 16, KW), F32), vm((4, 8, KW), F32), vm((4, 8, KW), F32),
                vm((3, 16, KW), F32), vm((3, 8, KW), F32), vm((3, 8, KW), F32),
                *[vm((2, 4, cap, CHUNK), F32) for cap in CAP],
                *[vm((2, 3, cap, CHUNK), F32) for cap in CAP],
                vm((3, 4 * CAP[0], CHUNK), BF16),
                vm((8, 128), F32), vm((8, 128), F32), vm((2, 2, 16, 16, 256), F32),
                dma((4,)), dma, dma((9,)), dma((9,)), dma((18,)), dma((18,)), dma, dma, dma((64,)), dma((64,)),
            ],
            compiler_params=pltpu.CompilerParams(vmem_limit_bytes=40 << 20, collective_id=0, has_side_effects=True),
            name="assemble",
        )(tokens, rows, *tables)
        flag = jnp.max(recv[:, 0, 255]) > 0.5

        def fast(_):
            vm, scalar = pl.BlockSpec(memory_space=pltpu.VMEM), pl.BlockSpec(memory_space=pltpu.SMEM)
            return pl.pallas_call(
                finish,
                out_shape=(shaped(*shard), shaped(*shard), shaped(*shard), shaped(*shard, dtype=BF16)),
                in_specs=[scalar, scalar, vm, vm, vm, vm, vm],
                out_specs=(vm, vm, vm, vm),
                scratch_shapes=[pltpu.VMEM(((shard_rows + 127) // 128, 16, 128), F32)],
                compiler_params=pltpu.CompilerParams(vmem_limit_bytes=VLIM),
                name="finish",
            )(learn_rate.reshape(1, 1), clip_scale.reshape(1, 1), recv, *near)

        def slow(_):
            grad = dense_grad(tokens.reshape(1, -1), rows, shard_rows)
            new_w, new_m, new_v = update_math(grad, *tables, learn_rate, clip_scale)
            return new_w, new_m, new_v, new_w.astype(BF16)

        return tuple(a.T for a in lax.cond(flag, slow, fast, None))

    return jax.shard_map(local_step, mesh=mesh, in_specs=(row_spec, act_spec, table_spec, table_spec, table_spec, table_spec, P(), P()), out_specs=(table_spec, table_spec, table_spec, table_spec), check_vma=False)
```
